256 devices in a mesh: ens: 4 (over x), slab: 64 (over y, z, core).
Axes of the slice: x: 4, y: 4, z: 8, core: 2. Of those that a mesh axis runs over, the one named last changes fastest.
Arguments:
- velocity: float32 [4, 3, 8, 2048, 1024], P('ens', None, None, 'slab'), may hold values from -6 to 6
- cutoffs: int32 [4, 2, 8], P('ens'), may hold values from 128 to 511, as said below
- plane_index: int32 [4], P('ens'), may hold values from 0 to 2047
- boundary_index: int32 [4], P('ens'), may hold values from 0 to 2047
Outputs:
- blended: float32 [4, 3, 8, 2048, 1024], P('ens', None, None, 'slab')
The draws below stay inside these ranges and needn't reach their ends.
Inputs may be any that keep to these rules, and one draw needn't show every extreme that they name: `cutoffs`: row 0 lies in 256 to 511 and row 1 in 128 to 255; in every member some level has row 0 equal to 511 and some level has row 1 equal to 255.
All inputs are finite; a program needn't handle non-finite values.
Results may differ from the reference program's by a relative error of at most 0.0003.
Values sent between devices are 32-bit elements; how exact they have to be, the bound alone decides.
A program may use at most 128 MiB of HBM per device.

```python
import jax
import jax.numpy as jnp
from jax import lax

NX = 2048
NY = 1024
KX = 512
KY = 256
COMP = 3
Z = 8
ENS = 4
N_ENS = 4


def draw_cutoffs(key, part):
    key_x, key_y, key_a, key_b = jax.random.split(jax.random.fold_in(key, 17), 4)
    levels = jnp.arange(Z, dtype=jnp.int32)
    cut_x = jax.random.randint(key_x, (N_ENS, Z), KX // 2, KX, dtype=jnp.int32)
    cut_y = jax.random.randint(key_y, (N_ENS, Z), KY // 2, KY, dtype=jnp.int32)
    top_x = jax.random.randint(key_a, (N_ENS, 1), 0, Z, dtype=jnp.int32)
    top_y = jax.random.randint(key_b, (N_ENS, 1), 0, Z, dtype=jnp.int32)
    cut_x = jnp.where(levels[None, :] == top_x, KX - 1, cut_x)
    cut_y = jnp.where(levels[None, :] == top_y, KY - 1, cut_y)
    return jnp.stack([cut_x, cut_y], axis=1).astype(jnp.int32)


def with_ends(values, rng, least, high):
    longest = values.shape.index(max(values.shape))
    spots = []
    for shift in (0, 1):
        where = [jax.random.randint(jax.random.fold_in(rng, axis), (), 0, length) for axis, length in enumerate(values.shape)]
        where[longest] = (where[longest] + shift) % values.shape[longest]
        spots.append(tuple(where))
    return values.at[spots[0]].set(least).at[spots[1]].set(high)


def level_of(stream_key, shape, cuts, low, high):
    gain, own = 1.0, jax.random.fold_in(stream_key, 6)
    for axis_at, blocks in cuts:
        steps = jnp.exp(jax.random.uniform(jax.random.fold_in(own, axis_at), (blocks,), jnp.float32, low / len(cuts), high / len(cuts)))
        gain = gain * jnp.repeat(steps, shape[axis_at] // blocks).reshape([-1 if axis == axis_at else 1 for axis in range(len(shape))])
    return gain


def bell_draw(stream_key, shape, deviation, bound, shards=(), kind=jnp.bfloat16):
    array = deviation * jax.random.normal(stream_key, shape, jnp.float32)
    if shards:
        array = array * level_of(stream_key, shape, shards, -0.22, 0.18)
    return jnp.clip(array, -bound, bound).astype(kind)


def setup_inputs(seed: int = 0) -> dict:
    splits = jax.random.split(jax.random.key(seed), 5)
    velocity = bell_draw(splits[0], (ENS, COMP, Z, NX, NY), 1.0, 6.0, ((0, 4), (3, 64)), jnp.float32)
    cutoffs = draw_cutoffs(jax.random.fold_in(splits[4], 71), 0)
    plane_index = with_ends(jax.random.randint(splits[2], (ENS,), 0, NX), jax.random.fold_in(splits[2], 1), 0, NX - 1).astype(jnp.int32)
    boundary_index = with_ends(jax.random.randint(splits[3], (ENS,), 0, NX), jax.random.fold_in(splits[3], 1), 0, NX - 1).astype(jnp.int32)
    return dict(velocity=velocity, cutoffs=cutoffs, plane_index=plane_index, boundary_index=boundary_index)


def filter_one(member_item):
    grid_values, cut_x, cut_y = member_item
    spectrum = jnp.fft.fft2(grid_values)
    wave_x = jnp.arange(NX, dtype=jnp.int32)
    wave_y = jnp.arange(NY, dtype=jnp.int32)
    kabs_x = jnp.minimum(wave_x, NX - wave_x)
    kabs_y = jnp.minimum(wave_y, NY - wave_y)
    keep = (kabs_x[:, None] <= cut_x) & (kabs_y[None, :] <= cut_y)
    kept = jnp.where(keep, spectrum, jnp.zeros_like(spectrum))
    return jnp.real(jnp.fft.ifft2(kept)).astype(grid_values.dtype)


def pick_plane(member_field, index_value):
    return lax.dynamic_index_in_dim(member_field, index_value.astype(jnp.int32), 2, keepdims=False)


def reference(velocity, cutoffs, plane_index, boundary_index):
    stacked = velocity.reshape(-1, NX, NY)
    cut_x = jnp.broadcast_to(cutoffs[:, 0][:, None, :], (N_ENS, COMP, Z)).reshape(-1)
    cut_y = jnp.broadcast_to(cutoffs[:, 1][:, None, :], (N_ENS, COMP, Z)).reshape(-1)
    filtered = lax.map(filter_one, (stacked, cut_x, cut_y)).reshape(velocity.shape)
    planes = jax.vmap(pick_plane)(filtered, plane_index)
    inflow = jnp.roll(planes, 1, axis=0)
    streamwise = jnp.arange(NX, dtype=jnp.int32)
    offset = jnp.abs(streamwise[None, :] - boundary_index.astype(jnp.int32)[:, None])
    distance = jnp.minimum(offset, NX - offset)
    relax = jnp.exp(-distance.astype(filtered.dtype) / (NX / 4.0))
    weight = relax[:, None, None, :, None]
    return filtered + weight * (inflow[:, :, :, None, :] - filtered)
```

```python
import functools

import jax
import jax.numpy as jnp
import ml_dtypes
import numpy as np
from jax import lax
from jax.experimental import pallas as pl
from jax.experimental.pallas import tpu as pltpu
from jax.sharding import PartitionSpec as P

MESH = pl.DeviceIdType.MESH
KX = 512
KY = 256
SLABS = 64
F32 = jnp.float32
BF16 = jnp.bfloat16


def split_table(table):
    high = table.astype(ml_dtypes.bfloat16)
    low = (table - high.astype(np.float64)).astype(ml_dtypes.bfloat16)
    return np.stack([high, low])


def half_basis(length, modes):
    position = np.arange(length // 2)
    tables = []
    for parity in (0, 1):
        wavenum = np.arange(parity, modes, 2)
        angles = (position[:, None] * wavenum[None, :] % length) * (2.0 * np.pi / length)
        tables.append(split_table(np.concatenate([np.cos(angles), np.sin(angles)], axis=1)))
    return np.stack(tables)


def dot(a, b):
    return lax.dot_general(a, b, (((1,), (0,)), ((), ())), preferred_element_type=F32)


def dot_nt(a, b):
    return lax.dot_general(a, b, (((1,), (1,)), ((), ())), preferred_element_type=F32)


def split(value):
    high = value.astype(BF16)
    return high, (value - high.astype(F32)).astype(BF16)


def exchange_groups(parts):
    lane = lax.broadcasted_iota(jnp.int32, parts[0].shape, parts[0].ndim - 1)
    axis = parts[0].ndim - 1
    for bit, width in ((1, 32), (2, 64)):
        first = (lane // width) % 2 == 0
        done = list(parts)
        for a in range(4):
            if a & bit:
                continue
            u, v = parts[a], parts[a | bit]
            done[a] = jnp.where(first, u, pltpu.roll(v, width, axis))
            done[a | bit] = jnp.where(first, pltpu.roll(u, 128 - width, axis), v)
        parts = done
    return parts


def filter_kernel(
    vel, cut, plane, bound, ytab, xtab, xtab_t,
    ret,
    u, yt, xt, xtt, spec, recv, data, mask, coef, parts, field, back, relax, plane_out, plane_in,
    load, table, send_f, recv_f, send_r, recv_r, send_p, recv_p,
):
    ens = lax.axis_index("ens")
    me = lax.axis_index("slab")
    my_y, my_z, my_c = lax.div(me, 16), lax.rem(lax.div(me, 2), 8), lax.rem(me, 2)
    after, before = lax.rem(ens + 1, 4), lax.rem(ens + 3, 4)

    def other(i):
        y = lax.rem(my_y + lax.rem(lax.div(i, 2), 4), 4)
        z = lax.rem(my_z + lax.div(i, 8), 8)
        c = lax.rem(my_c + lax.rem(i, 2), 2)
        return y * 16 + z * 2 + c

    loads = [pltpu.make_async_copy(vel.at[c], u.at[c], load.at[c]) for c in range(3)]
    tables = [pltpu.make_async_copy(a, b, table.at[i]) for i, (a, b) in enumerate(((ytab, yt), (xtab, xt), (xtab_t, xtt)))]
    loads[0].start()
    tables[0].start()

    barrier = pltpu.get_barrier_semaphore()

    def greet(i, _):
        pl.semaphore_signal(barrier, 1, device_id={"ens": ens, "slab": other(i)}, device_id_type=MESH)
        return 0

    lax.fori_loop(1, SLABS, greet, 0)
    for e in (after, before):
        pl.semaphore_signal(barrier, 1, device_id={"ens": e, "slab": me}, device_id_type=MESH)
    for copy in (loads[1], loads[2], tables[1], tables[2]):
        copy.start()

    def spread(source, target, c, sent, landed):
        def one(i, _):
            t = other(i)
            pltpu.make_async_remote_copy(
                source.at[c, t], target.at[c, me], sent.at[c], landed.at[c],
                device_id={"ens": ens, "slab": t}, device_id_type=MESH,
            ).start()
            return 0

        lax.fori_loop(1, SLABS, one, 0)

    def all_of(buffer, c, sem):
        blocks = buffer.at[c, pl.ds(0, SLABS - 1)]
        pltpu.make_async_copy(blocks, blocks, sem.at[c]).wait()

    def analyse(c):
        pltpu.make_async_copy(vel.at[c], u.at[c], load.at[c]).wait()
        left, right = u[c, :, :512], u[c, :, 512:]
        for parity in (0, 1):
            high, low = split(left + right if parity == 0 else left - right)
            total = dot_nt(yt[parity, 0], high) + (dot_nt(yt[parity, 0], low) + dot_nt(yt[parity, 1], high))
            spec[c, pl.ds(32 * parity, 32)] = total.reshape(32, 8, 256)

    tables[0].wait()
    analyse(0)
    pl.semaphore_wait(barrier, SLABS + 1)

    def forward(c, _):
        @pl.when(c > 0)
        def _():
            analyse(c)

        spread(spec, recv, c, send_f, recv_f)
        recv[c, me] = spec[c, me]
        return 0

    lax.fori_loop(0, 3, forward, 0)

    row = lax.broadcasted_iota(jnp.int32, (8, 512), 0)
    column = lax.broadcasted_iota(jnp.int32, (8, 512), 1)
    ky = 2 * ((8 * me + row) % 128) + lax.div(me, 32)
    weight_y = jnp.where(ky == 0, 1.0, 2.0) / 1024.0
    for parity in (0, 1):
        kx = 2 * (column % 256) + parity
        weight = weight_y * (jnp.where(kx == 0, 1.0, 2.0) / 2048.0)
        for z in range(8):
            kept = jnp.logical_and(kx <= cut[0, z], ky <= cut[1, z])
            mask[parity, pl.ds(8 * z, 8), :] = jnp.where(kept, weight, 0.0)
    lane = lax.broadcasted_iota(jnp.int32, (8, 128), 1)
    for q in range(16):
        offset = jnp.abs(128 * q + lane - bound[0])
        distance = jnp.minimum(offset, 2048 - offset)
        relax[q] = jnp.exp(-distance.astype(F32) / 512.0)
    tables[1].wait()
    tables[2].wait()

    def filter_chunk(c, _):
        all_of(recv, c, recv_f)

        def gather(q, _):
            at = pl.ds(pl.multiple_of(128 * q, 128), 128)
            for h in (0, 1):
                pieces = [(recv[c, 4 * q + a, :, pl.ds(128 * h, 128)], recv[c, 32 + 4 * q + a, :, pl.ds(128 * h, 128)]) for a in range(4)]
                for parity in (0, 1):
                    mixed = exchange_groups([m + n if parity == 0 else m - n for m, n in pieces])
                    high, low = split(jnp.concatenate(mixed, axis=0))
                    data[parity, pl.ds(32 * h, 32), at] = high
                    data[parity, pl.ds(64 + 32 * h, 32), at] = low
            return 0

        lax.fori_loop(0, 8, gather, 0)
        for parity in (0, 1):
            both = dot(data[parity], xt[parity, 0])
            kept = (both[:64] + (both[64:] + dot(data[parity, :64], xt[parity, 1]))) * mask[parity]
            high, low = split(kept)
            coef[:64] = high
            coef[64:] = low
            both = dot(coef[...], xtt[parity, 0])
            parts[parity] = both[:64] + (both[64:] + dot(coef[:64], xtt[parity, 1]))

        xi = lax.broadcasted_iota(jnp.int32, (64, 128), 1)

        def combine(q, picked):
            at = pl.ds(pl.multiple_of(128 * q, 128), 128)
            even, odd = parts[0, :, at], parts[1, :, at]
            near, far = even + odd, even - odd
            field[0, :, at] = near
            field[1, :, at] = far
            x = xi + 128 * q
            return picked + (jnp.where(x == plane[0], near, 0.0) + jnp.where(x + 1024 == plane[0], far, 0.0))

        picked = lax.fori_loop(0, 8, combine, jnp.zeros((64, 128), F32))
        plane_out[c] = jnp.broadcast_to(jnp.sum(picked, axis=1, keepdims=True), (64, 128))
        handed = pltpu.make_async_remote_copy(
            plane_out.at[c], plane_in.at[c], send_p.at[c], recv_p.at[c],
            device_id={"ens": after, "slab": me}, device_id_type=MESH,
        )
        handed.start()
        handed.wait_recv()

        def scatter(q, _):
            at = pl.ds(pl.multiple_of(128 * q, 128), 128)
            for half in (0, 1):
                weight = relax[8 * half + q]
                for h in (0, 1):
                    rows = []
                    for b in range(4):
                        own = field[half, pl.ds(32 * h + 8 * b, 8), at]
                        rows.append(own + weight * (plane_in[c, pl.ds(32 * h + 8 * b, 8), :] - own))
                    for a, piece in enumerate(exchange_groups(rows)):
                        back[c, 32 * half + 4 * q + a, :, pl.ds(128 * h, 128)] = piece
            return 0

        lax.fori_loop(0, 8, scatter, 0)
        spread(back, ret, c, send_r, recv_r)
        ret[c, me] = back[c, me]
        return 0

    lax.fori_loop(0, 3, filter_chunk, 0)

    def finish(c, _):
        all_of(recv, c, send_f)
        all_of(recv, c, send_r)
        all_of(recv, c, recv_r)
        pltpu.make_async_copy(plane_out.at[c], plane_out.at[c], send_p.at[c]).wait()
        return 0

    lax.fori_loop(0, 3, finish, 0)


def synthesis_kernel(ret, yt, out):
    halves = []
    for parity in (0, 1):
        high, low = split(ret[0, pl.ds(256 * parity, 256), :].T)
        halves.append(dot(high, yt[parity, 0]) + (dot(low, yt[parity, 0]) + dot(high, yt[parity, 1])))
    out[0, :, :512] = halves[0] + halves[1]
    out[0, :, 512:] = halves[0] - halves[1]


def on_device(velocity, cutoffs, plane_index, boundary_index):
    ytab = jnp.asarray(np.ascontiguousarray(half_basis(1024, KY).transpose(0, 1, 3, 2)))
    x_basis = half_basis(2048, KX)
    xtab = jnp.asarray(x_basis)
    xtab_t = jnp.asarray(np.ascontiguousarray(x_basis.transpose(0, 1, 3, 2)))
    anywhere = pl.BlockSpec(memory_space=pltpu.HBM)
    smem = pl.BlockSpec(memory_space=pltpu.SMEM)
    dma = pltpu.SemaphoreType.DMA
    blocks = pltpu.VMEM((3, SLABS, 8, 256), F32)
    ret = pl.pallas_call(
        filter_kernel,
        out_shape=jax.ShapeDtypeStruct((3, SLABS, 8, 256), F32),
        in_specs=[anywhere, smem, smem, smem, anywhere, anywhere, anywhere],
        out_specs=pl.BlockSpec(memory_space=pltpu.VMEM),
        scratch_shapes=[
            pltpu.VMEM((3, 256, 1024), F32),
            pltpu.VMEM(ytab.shape, BF16),
            pltpu.VMEM(xtab.shape, BF16),
            pltpu.VMEM(xtab_t.shape, BF16),
            blocks,
            blocks,
            pltpu.VMEM((2, 128, 1024), BF16),
            pltpu.VMEM((2, 64, 512), F32),
            pltpu.VMEM((128, 512), BF16),
            pltpu.VMEM((2, 64, 1024), F32),
            pltpu.VMEM((2, 64, 1024), F32),
            blocks,
            pltpu.VMEM((16, 8, 128), F32),
            pltpu.VMEM((3, 64, 128), F32),
            pltpu.VMEM((3, 64, 128), F32),
        ]
        + [dma((3,))] * 8,
        compiler_params=pltpu.CompilerParams(collective_id=0, has_side_effects=True, vmem_limit_bytes=48 << 20),
    )(velocity.reshape(3, 256, 1024), cutoffs[0], plane_index, boundary_index, ytab, xtab, xtab_t)
    out = pl.pallas_call(
        synthesis_kernel,
        grid=(3,),
        out_shape=jax.ShapeDtypeStruct((3, 256, 1024), F32),
        in_specs=[
            pl.BlockSpec((1, 512, 256), lambda i: (i, 0, 0)),
            pl.BlockSpec(ytab.shape, lambda i: (0, 0, 0, 0)),
        ],
        out_specs=pl.BlockSpec((1, 256, 1024), lambda i: (i, 0, 0)),
    )(ret.reshape(3, 512, 256), ytab)
    return out.reshape(velocity.shape)


def solution(mesh):
    in_specs = (P("ens", None, None, "slab", None), P("ens", None, None), P("ens"), P("ens"))
    out_specs = P("ens", None, None, "slab", None)
    return jax.shard_map(on_device, mesh=mesh, in_specs=in_specs, out_specs=out_specs, check_vma=False)
```

```python
import functools

import jax
import jax.numpy as jnp
import ml_dtypes
import numpy as np
from jax import lax
from jax.experimental import pallas as pl
from jax.experimental.pallas import tpu as pltpu
from jax.sharding import PartitionSpec as P

MESH = pl.DeviceIdType.MESH
KX = 512
KY = 256
SLABS = 64
VMEM_GRANT = 36 << 20
AT_Y, AT_X, AT_XT = pl.ds(0, 2), pl.ds(2, 8), pl.ds(10, 8)
F32 = jnp.float32
BF16 = jnp.bfloat16


def split_table(table):
    high = table.astype(ml_dtypes.bfloat16)
    low = (table - high.astype(np.float64)).astype(ml_dtypes.bfloat16)
    return np.stack([high, low])


def half_basis(length, modes):
    position = np.arange(length // 2)
    tables = []
    for parity in (0, 1):
        wavenum = np.arange(parity, modes, 2)
        angles = (position[:, None] * wavenum[None, :] % length) * (2.0 * np.pi / length)
        tables.append(split_table(np.concatenate([np.cos(angles), np.sin(angles)], axis=1)))
    return np.stack(tables)


def dot(a, b):
    return lax.dot_general(a, b, (((1,), (0,)), ((), ())), preferred_element_type=F32)


def dot_nt(a, b):
    return lax.dot_general(a, b, (((1,), (1,)), ((), ())), preferred_element_type=F32)


def split(value):
    high = value.astype(BF16)
    return high, (value - high.astype(F32)).astype(BF16)


def synthesise(coefficients, tab_y, out):
    halves = []
    for parity in (0, 1):
        y_high, y_low = tab_y[parity, :256], tab_y[parity, 256:]
        high, low = split(coefficients[256 * parity : 256 * parity + 256].T)
        halves.append(dot(high, y_high) + (dot(low, y_high) + dot(high, y_low)))
    out[:, :512] = halves[0] + halves[1]
    out[:, 512:] = halves[0] - halves[1]


def exchange_groups(parts):
    lane = lax.broadcasted_iota(jnp.int32, parts[0].shape, parts[0].ndim - 1)
    axis = parts[0].ndim - 1
    for bit, width in ((1, 32), (2, 64)):
        first = (lane // width) % 2 == 0
        done = list(parts)
        for a in range(4):
            if a & bit:
                continue
            u, v = parts[a], parts[a | bit]
            done[a] = jnp.where(first, u, pltpu.roll(v, width, axis))
            done[a | bit] = jnp.where(first, pltpu.roll(u, 128 - width, axis), v)
        parts = done
    return parts


def filter_kernel(
    vel, cut_at, plane, bound, tables,
    first_out, second_out, last_out, tab_y,
    cut, u, tab, spec, recv, data, mask, coef, parts, field, back, ret, ret_half, relax, plane_out, plane_in,
    scalar, load, table, send_f, recv_f, send_r, recv_r, send_p, recv_p,
):
    ens = lax.axis_index("ens")
    me = lax.axis_index("slab")
    my_y, my_z, my_c = lax.div(me, 16), lax.rem(lax.div(me, 2), 8), lax.rem(me, 2)
    after, before = lax.rem(ens + 1, 4), lax.rem(ens + 3, 4)

    def other(i):
        i = i - 1
        step = lax.div(i, 8)
        dz = lax.rem(12 + (1 - 2 * lax.rem(step, 2)) * lax.div(step + 1, 2), 8)
        dy, dc = 3 - lax.rem(lax.div(i, 2), 4), 1 - lax.rem(i, 2)
        return lax.rem(my_y + dy, 4) * 16 + lax.rem(my_z + dz, 8) * 2 + lax.rem(my_c + dc, 2)

    loads = [pltpu.make_async_copy(vel.at[c], u.at[c], load.at[c]) for c in range(3)]
    bases = [
        pltpu.make_async_copy(tables.at[AT_Y], tab_y, table.at[0]),
        pltpu.make_async_copy(tables.at[AT_X], tab.at[pl.ds(0, 8)], table.at[1]),
        pltpu.make_async_copy(tables.at[AT_XT], tab.at[pl.ds(8, 8)], table.at[2]),
    ]
    limits = pltpu.make_async_copy(cut_at, cut, scalar)
    loads[0].start()
    bases[0].start()

    barrier = pltpu.get_barrier_semaphore()

    def greet(i, _):
        pl.semaphore_signal(barrier, 1, device_id={"ens": ens, "slab": other(i)}, device_id_type=MESH)
        return 0

    lax.fori_loop(1, SLABS, greet, 0)
    for e in (after, before):
        pl.semaphore_signal(barrier, 1, device_id={"ens": e, "slab": me}, device_id_type=MESH)
    for copy in (loads[1], loads[2], bases[1], bases[2], limits):
        copy.start()

    def spread(source, target, c, sent, landed):
        def one(i, _):
            t = other(i)
            pltpu.make_async_remote_copy(
                source.at[c, t], target.at[c, me], sent.at[c], landed.at[c],
                device_id={"ens": ens, "slab": t}, device_id_type=MESH,
            ).start()
            return 0

        lax.fori_loop(1, SLABS, one, 0)

    def all_of(buffer, c, sem):
        blocks = buffer.at[c, pl.ds(0, SLABS - 1)]
        pltpu.make_async_copy(blocks, blocks, sem.at[c]).wait()

    def half_of(buffer, h, sem):
        blocks = buffer.at[pl.ds(0, SLABS - 1)]
        pltpu.make_async_copy(blocks, blocks, sem.at[2 + h]).wait()

    def spread_half(source, target, h, sent, landed):
        def one(i, _):
            t = other(i)
            pltpu.make_async_remote_copy(
                source.at[2, t, :, pl.ds(128 * h, 128)], target.at[me], sent.at[2 + h], landed.at[2 + h],
                device_id={"ens": ens, "slab": t}, device_id_type=MESH,
            ).start()
            return 0

        lax.fori_loop(1, SLABS, one, 0)

    def analyse(c):
        pltpu.make_async_copy(vel.at[c], u.at[c], load.at[c]).wait()
        left, right = u[c, :, :512], u[c, :, 512:]
        for parity in (0, 1):
            high, low = split(left + right if parity == 0 else left - right)
            y_high, y_low = tab_y[parity, :256], tab_y[parity, 256:]
            total = dot_nt(y_high, high) + (dot_nt(y_high, low) + dot_nt(y_low, high))
            spec[c, pl.ds(32 * parity, 32)] = total.reshape(32, 8, 256)

    bases[0].wait()
    analyse(0)
    pl.semaphore_wait(barrier, SLABS + 1)

    def forward(c, _):
        @pl.when(c > 0)
        def _():
            analyse(c)

        spread(spec, recv, c, send_f, recv_f)
        recv[c, me] = spec[c, me]
        return 0

    lax.fori_loop(0, 3, forward, 0)

    limits.wait()
    row = lax.broadcasted_iota(jnp.int32, (8, 512), 0)
    column = lax.broadcasted_iota(jnp.int32, (8, 512), 1)
    ky = 2 * ((8 * me + row) % 128) + lax.div(me, 32)
    weight_y = jnp.where(ky == 0, 1.0, 2.0) / 1024.0
    for parity in (0, 1):
        kx = 2 * (column % 256) + parity
        weight = weight_y * (jnp.where(kx == 0, 1.0, 2.0) / 2048.0)
        for z in range(8):
            kept = jnp.logical_and(kx <= cut[0, 0, z], ky <= cut[0, 1, z])
            mask[parity, pl.ds(8 * z, 8), :] = jnp.where(kept, weight, 0.0)
    lane = lax.broadcasted_iota(jnp.int32, (8, 128), 1)
    for q in range(16):
        offset = jnp.abs(128 * q + lane - bound[0])
        distance = jnp.minimum(offset, 2048 - offset)
        relax[q] = jnp.exp(-distance.astype(F32) / 512.0)
    bases[1].wait()
    bases[2].wait()

    def filter_chunk(c, _):
        all_of(recv, c, recv_f)

        def gather(q, _):
            at = pl.ds(pl.multiple_of(128 * q, 128), 128)
            for h in (0, 1):
                pieces = [(recv[c, 4 * q + a, :, pl.ds(128 * h, 128)], recv[c, 32 + 4 * q + a, :, pl.ds(128 * h, 128)]) for a in range(4)]
                for parity in (0, 1):
                    mixed = exchange_groups([m + n if parity == 0 else m - n for m, n in pieces])
                    high, low = split(jnp.concatenate(mixed, axis=0))
                    data[parity, pl.ds(32 * h, 32), at] = high
                    data[parity, pl.ds(64 + 32 * h, 32), at] = low
            return 0

        lax.fori_loop(0, 8, gather, 0)
        for parity in (0, 1):
            x_high, x_low = (tab[pl.ds(4 * parity + 2 * i, 2)].reshape(1024, 512) for i in (0, 1))
            both = dot(data[parity], x_high)
            kept = (both[:64] + (both[64:] + dot(data[parity, :64], x_low))) * mask[parity]
            high, low = split(kept)
            coef[:64] = high
            coef[64:] = low
            for side in (0, 1):
                both = dot(coef[...], tab[8 + 4 * parity + side])
                low = dot(coef[:64], tab[10 + 4 * parity + side])
                parts[parity, :, pl.ds(512 * side, 512)] = both[:64] + (both[64:] + low)

        xi = lax.broadcasted_iota(jnp.int32, (64, 128), 1)

        def combine(q, picked):
            at = pl.ds(pl.multiple_of(128 * q, 128), 128)
            even, odd = parts[0, :, at], parts[1, :, at]
            near, far = even + odd, even - odd
            field[0, :, at] = near
            field[1, :, at] = far
            x = xi + 128 * q
            return picked + (jnp.where(x == plane[0], near, 0.0) + jnp.where(x + 1024 == plane[0], far, 0.0))

        picked = lax.fori_loop(0, 8, combine, jnp.zeros((64, 128), F32))
        plane_out[c] = jnp.broadcast_to(jnp.sum(picked, axis=1, keepdims=True), (64, 128))
        handed = pltpu.make_async_remote_copy(
            plane_out.at[c], plane_in.at[c], send_p.at[c], recv_p.at[c],
            device_id={"ens": after, "slab": me}, device_id_type=MESH,
        )
        handed.start()
        handed.wait_recv()

        def scatter(q, _):
            at = pl.ds(pl.multiple_of(128 * q, 128), 128)
            for half in (0, 1):
                weight = relax[8 * half + q]
                for h in (0, 1):
                    rows = []
                    for b in range(4):
                        own = field[half, pl.ds(32 * h + 8 * b, 8), at]
                        rows.append(own + weight * (plane_in[c, pl.ds(32 * h + 8 * b, 8), :] - own))
                    for a, piece in enumerate(exchange_groups(rows)):
                        back[c, 32 * half + 4 * q + a, :, pl.ds(128 * h, 128)] = piece
            return 0

        lax.fori_loop(0, 8, scatter, 0)

        @pl.when(c < 2)
        def _():
            spread(back, ret, c, send_r, recv_r)
            ret[c, me] = back[c, me]

        @pl.when(c == 2)
        def _():
            for h, target in enumerate((ret_half, last_out)):
                spread_half(back, target, h, send_r, recv_r)
                target[me] = back[2, me, :, pl.ds(128 * h, 128)]

        return 0

    lax.fori_loop(0, 3, filter_chunk, 0)

    def early(c, _):
        all_of(ret, c, recv_r)
        synthesise(ret[c].reshape(512, 256), tab_y, first_out.at[c])
        return 0

    lax.fori_loop(0, 2, early, 0)
    half_of(ret_half, 0, recv_r)
    synthesise(ret_half[...].reshape(512, 128), tab_y, second_out)

    def finish(c, _):
        all_of(spec, c, send_f)
        pltpu.make_async_copy(plane_out.at[c], plane_out.at[c], send_p.at[c]).wait()
        return 0

    lax.fori_loop(0, 3, finish, 0)
    for c in (0, 1):
        all_of(back, c, send_r)
    for h in (0, 1):
        half_of(ret_half, h, send_r)
    half_of(last_out, 1, recv_r)


def emit_kernel(first, second, last, tab_y, out, rest, sem):
    copies = [
        pltpu.make_async_copy(first, out.at[pl.ds(0, 2)], sem.at[0]),
        pltpu.make_async_copy(second, out.at[2, pl.ds(0, 128)], sem.at[1]),
        pltpu.make_async_copy(rest, out.at[2, pl.ds(128, 128)], sem.at[2]),
    ]
    copies[0].start()
    copies[1].start()
    synthesise(last[...].reshape(512, 128), tab_y, rest)
    copies[2].start()
    for copy in copies:
        copy.wait()


def in_hbm(array):
    return pltpu.with_memory_space_constraint(array, pltpu.HBM)


def on_device(velocity, cutoffs, plane_index, boundary_index):
    y_basis = half_basis(1024, KY).transpose(0, 1, 3, 2).reshape(2, 512, 512)
    x_basis = half_basis(2048, KX)
    x_back = x_basis.transpose(0, 1, 3, 2).reshape(2, 2, 512, 2, 512).transpose(0, 1, 3, 2, 4).reshape(8, 512, 512)
    tables = jnp.asarray(np.concatenate([y_basis, x_basis.reshape(8, 512, 512), x_back]))
    smem, vmem = pltpu.SMEM, pltpu.VMEM
    here = pl.BlockSpec(memory_space=vmem)
    anywhere = pl.BlockSpec(memory_space=pl.ANY)
    dma = pltpu.SemaphoreType.DMA
    blocks = vmem((3, SLABS, 8, 256), F32)
    scalar = pl.BlockSpec(memory_space=smem)
    pieces = pl.pallas_call(
        filter_kernel,
        out_shape=[
            jax.ShapeDtypeStruct((2, 256, 1024), F32),
            jax.ShapeDtypeStruct((128, 1024), F32),
            jax.ShapeDtypeStruct((SLABS, 8, 128), F32),
            jax.ShapeDtypeStruct((2, 512, 512), BF16),
        ],
        in_specs=[anywhere, anywhere, scalar, scalar, anywhere],
        out_specs=[here] * 4,
        scratch_shapes=[
            smem((1, 2, 8), jnp.int32),
            vmem((3, 256, 1024), F32),
            vmem((16, 512, 512), BF16),
            blocks,
            blocks,
            vmem((2, 128, 1024), BF16),
            vmem((2, 64, 512), F32),
            vmem((128, 512), BF16),
            vmem((2, 64, 1024), F32),
            vmem((2, 64, 1024), F32),
            blocks,
            vmem((2, SLABS, 8, 256), F32),
            vmem((SLABS, 8, 128), F32),
            vmem((16, 8, 128), F32),
            vmem((3, 64, 128), F32),
            vmem((3, 64, 128), F32),
        ]
        + [dma] + [dma((n,)) for n in (3, 3, 3, 3, 4, 4, 3, 3)],
        compiler_params=pltpu.CompilerParams(collective_id=0, has_side_effects=True, vmem_limit_bytes=VMEM_GRANT),
    )(in_hbm(velocity.reshape(3, 256, 1024)), in_hbm(cutoffs), plane_index, boundary_index, in_hbm(tables))
    out = pl.pallas_call(
        emit_kernel,
        out_shape=jax.ShapeDtypeStruct((3, 256, 1024), F32),
        in_specs=[here] * 4,
        out_specs=anywhere,
        scratch_shapes=[vmem((128, 1024), F32), dma((3,))],
        compiler_params=pltpu.CompilerParams(vmem_limit_bytes=16 << 20),
    )(*pieces)
    return out.reshape(velocity.shape)


def solution(mesh):
    in_specs = (P("ens", None, None, "slab", None), P("ens", None, None), P("ens"), P("ens"))
    out_specs = P("ens", None, None, "slab", None)
    return jax.shard_map(on_device, mesh=mesh, in_specs=in_specs, out_specs=out_specs, check_vma=False)
```

```python
import functools

import jax
import jax.numpy as jnp
import ml_dtypes
import numpy as np
from jax import lax
from jax.experimental import pallas as pl
from jax.experimental.pallas import tpu as pltpu
from jax.sharding import PartitionSpec as P

MESH = pl.DeviceIdType.MESH
KX = 512
KY = 256
SLABS = 64
VMEM_GRANT = 36 << 20
AT_Y, AT_X, AT_XT = pl.ds(0, 2), pl.ds(2, 8), pl.ds(10, 8)
F32 = jnp.float32
BF16 = jnp.bfloat16


def split_table(table):
    high = table.astype(ml_dtypes.bfloat16)
    low = (table - high.astype(np.float64)).astype(ml_dtypes.bfloat16)
    return np.stack([high, low])


def half_basis(length, modes):
    position = np.arange(length // 2)
    tables = []
    for parity in (0, 1):
        wavenum = np.arange(parity, modes, 2)
        angles = (position[:, None] * wavenum[None, :] % length) * (2.0 * np.pi / length)
        tables.append(split_table(np.concatenate([np.cos(angles), np.sin(angles)], axis=1)))
    return np.stack(tables)


def dot(a, b):
    return lax.dot_general(a, b, (((1,), (0,)), ((), ())), preferred_element_type=F32)


def dot_nt(a, b):
    return lax.dot_general(a, b, (((1,), (1,)), ((), ())), preferred_element_type=F32)


def split(value):
    high = value.astype(BF16)
    return high, (value - high.astype(F32)).astype(BF16)


def synthesise(coefficients, tab_y, out):
    halves = []
    for parity in (0, 1):
        y_high, y_low = tab_y[parity, :256], tab_y[parity, 256:]
        high, low = split(coefficients[256 * parity : 256 * parity + 256].T)
        halves.append(dot(high, y_high) + (dot(low, y_high) + dot(high, y_low)))
    out[:, :512] = halves[0] + halves[1]
    out[:, 512:] = halves[0] - halves[1]


def exchange_groups(parts):
    lane = lax.broadcasted_iota(jnp.int32, parts[0].shape, parts[0].ndim - 1)
    axis = parts[0].ndim - 1
    for bit, width in ((1, 32), (2, 64)):
        first = (lane // width) % 2 == 0
        done = list(parts)
        for a in range(4):
            if a & bit:
                continue
            u, v = parts[a], parts[a | bit]
            done[a] = jnp.where(first, u, pltpu.roll(v, width, axis))
            done[a | bit] = jnp.where(first, pltpu.roll(u, 128 - width, axis), v)
        parts = done
    return parts


def filter_kernel(
    vel, cut_at, plane, bound, tables,
    first_out, second_out, last_out, tab_y,
    cut, u, tab, spec, recv, data, mask, coef, parts, field, back, ret, ret_half, relax, plane_out, plane_in,
    scalar, load, table, send_f, recv_f, send_r, recv_r, send_p, recv_p,
):
    ens = lax.axis_index("ens")
    me = lax.axis_index("slab")
    my_y, my_z, my_c = lax.div(me, 16), lax.rem(lax.div(me, 2), 8), lax.rem(me, 2)
    after, before = lax.rem(ens + 1, 4), lax.rem(ens + 3, 4)

    def other(i):
        i = i - 1
        step = lax.div(i, 8)
        dz = lax.rem(12 + (1 - 2 * lax.rem(step, 2)) * lax.div(step + 1, 2), 8)
        dy, dc = 3 - lax.rem(lax.div(i, 2), 4), 1 - lax.rem(i, 2)
        return lax.rem(my_y + dy, 4) * 16 + lax.rem(my_z + dz, 8) * 2 + lax.rem(my_c + dc, 2)

    def served(i):
        step = lax.div(i, 8)
        z = step + lax.div(step, 5) * (12 - 2 * step)
        return lax.rem(my_y + lax.rem(lax.div(i, 2), 4), 4) * 16 + z * 2 + lax.rem(my_c + lax.rem(i, 2), 2)

    loads = [pltpu.make_async_copy(vel.at[c], u.at[c], load.at[c]) for c in range(3)]
    bases = [
        pltpu.make_async_copy(tables.at[AT_Y], tab_y, table.at[0]),
        pltpu.make_async_copy(tables.at[AT_X], tab.at[pl.ds(0, 8)], table.at[1]),
        pltpu.make_async_copy(tables.at[AT_XT], tab.at[pl.ds(8, 8)], table.at[2]),
    ]
    limits = pltpu.make_async_copy(cut_at, cut, scalar)
    loads[0].start()
    bases[0].start()

    barrier = pltpu.get_barrier_semaphore()

    def greet(i, _):
        pl.semaphore_signal(barrier, 1, device_id={"ens": ens, "slab": other(i)}, device_id_type=MESH)
        return 0

    lax.fori_loop(1, SLABS, greet, 0)
    for e in (after, before):
        pl.semaphore_signal(barrier, 1, device_id={"ens": e, "slab": me}, device_id_type=MESH)
    for copy in (loads[1], loads[2], bases[1], bases[2], limits):
        copy.start()

    def spread(source, target, c, sent, landed):
        def one(i, _):
            t = other(i)
            pltpu.make_async_remote_copy(
                source.at[c, t], target.at[c, me], sent.at[c], landed.at[c],
                device_id={"ens": ens, "slab": t}, device_id_type=MESH,
            ).start()
            return 0

        lax.fori_loop(1, SLABS, one, 0)

    def all_of(buffer, c, sem):
        blocks = buffer.at[c, pl.ds(0, SLABS - 1)]
        pltpu.make_async_copy(blocks, blocks, sem.at[c]).wait()

    def half_of(buffer, h, sem):
        blocks = buffer.at[pl.ds(0, SLABS - 1)]
        pltpu.make_async_copy(blocks, blocks, sem.at[2 + h]).wait()

    def give_back(source, target, sent, landed):
        def one(i, _):
            t = served(i)

            @pl.when(t != me)
            def _():
                pltpu.make_async_remote_copy(
                    source(t), target.at[me], sent, landed, device_id={"ens": ens, "slab": t}, device_id_type=MESH
                ).start()

            return 0

        lax.fori_loop(0, SLABS, one, 0)

    def analyse(c):
        pltpu.make_async_copy(vel.at[c], u.at[c], load.at[c]).wait()
        left, right = u[c, :, :512], u[c, :, 512:]
        for parity in (0, 1):
            high, low = split(left + right if parity == 0 else left - right)
            y_high, y_low = tab_y[parity, :256], tab_y[parity, 256:]
            total = dot_nt(y_high, high) + (dot_nt(y_high, low) + dot_nt(y_low, high))
            spec[c, pl.ds(32 * parity, 32)] = total.reshape(32, 8, 256)

    bases[0].wait()
    analyse(0)
    pl.semaphore_wait(barrier, SLABS + 1)

    def forward(c, _):
        @pl.when(c > 0)
        def _():
            analyse(c)

        spread(spec, recv, c, send_f, recv_f)
        recv[c, me] = spec[c, me]
        return 0

    lax.fori_loop(0, 3, forward, 0)

    limits.wait()
    row = lax.broadcasted_iota(jnp.int32, (8, 512), 0)
    column = lax.broadcasted_iota(jnp.int32, (8, 512), 1)
    ky = 2 * ((8 * me + row) % 128) + lax.div(me, 32)
    weight_y = jnp.where(ky == 0, 1.0, 2.0) / 1024.0
    for parity in (0, 1):
        kx = 2 * (column % 256) + parity
        weight = weight_y * (jnp.where(kx == 0, 1.0, 2.0) / 2048.0)
        for z in range(8):
            kept = jnp.logical_and(kx <= cut[0, 0, z], ky <= cut[0, 1, z])
            mask[parity, pl.ds(8 * z, 8), :] = jnp.where(kept, weight, 0.0)
    lane = lax.broadcasted_iota(jnp.int32, (8, 128), 1)
    for q in range(16):
        offset = jnp.abs(128 * q + lane - bound[0])
        distance = jnp.minimum(offset, 2048 - offset)
        relax[q] = jnp.exp(-distance.astype(F32) / 512.0)
    bases[1].wait()
    bases[2].wait()

    def filter_chunk(c, _):
        all_of(recv, c, recv_f)

        def gather(q, _):
            at = pl.ds(pl.multiple_of(128 * q, 128), 128)
            for h in (0, 1):
                pieces = [(recv[c, 4 * q + a, :, pl.ds(128 * h, 128)], recv[c, 32 + 4 * q + a, :, pl.ds(128 * h, 128)]) for a in range(4)]
                for parity in (0, 1):
                    mixed = exchange_groups([m + n if parity == 0 else m - n for m, n in pieces])
                    high, low = split(jnp.concatenate(mixed, axis=0))
                    data[parity, pl.ds(32 * h, 32), at] = high
                    data[parity, pl.ds(64 + 32 * h, 32), at] = low
            return 0

        lax.fori_loop(0, 8, gather, 0)
        for parity in (0, 1):
            x_high, x_low = (tab[pl.ds(4 * parity + 2 * i, 2)].reshape(1024, 512) for i in (0, 1))
            both = dot(data[parity], x_high)
            kept = (both[:64] + (both[64:] + dot(data[parity, :64], x_low))) * mask[parity]
            high, low = split(kept)
            coef[:64] = high
            coef[64:] = low
            for side in (0, 1):
                both = dot(coef[...], tab[8 + 4 * parity + side])
                low = dot(coef[:64], tab[10 + 4 * parity + side])
                parts[parity, :, pl.ds(512 * side, 512)] = both[:64] + (both[64:] + low)

        xi = lax.broadcasted_iota(jnp.int32, (64, 128), 1)

        def combine(q, picked):
            at = pl.ds(pl.multiple_of(128 * q, 128), 128)
            even, odd = parts[0, :, at], parts[1, :, at]
            near, far = even + odd, even - odd
            field[0, :, at] = near
            field[1, :, at] = far
            x = xi + 128 * q
            return picked + (jnp.where(x == plane[0], near, 0.0) + jnp.where(x + 1024 == plane[0], far, 0.0))

        picked = lax.fori_loop(0, 8, combine, jnp.zeros((64, 128), F32))
        plane_out[c] = jnp.broadcast_to(jnp.sum(picked, axis=1, keepdims=True), (64, 128))
        handed = pltpu.make_async_remote_copy(
            plane_out.at[c], plane_in.at[c], send_p.at[c], recv_p.at[c],
            device_id={"ens": after, "slab": me}, device_id_type=MESH,
        )
        handed.start()
        handed.wait_recv()

        def scatter(q, _):
            at = pl.ds(pl.multiple_of(128 * q, 128), 128)
            for half in (0, 1):
                weight = relax[8 * half + q]
                for h in (0, 1):
                    rows = []
                    for b in range(4):
                        own = field[half, pl.ds(32 * h + 8 * b, 8), at]
                        rows.append(own + weight * (plane_in[c, pl.ds(32 * h + 8 * b, 8), :] - own))
                    for a, piece in enumerate(exchange_groups(rows)):
                        back[c, 32 * half + 4 * q + a, :, pl.ds(128 * h, 128)] = piece
            return 0

        lax.fori_loop(0, 8, scatter, 0)

        @pl.when(c < 2)
        def _():
            give_back(lambda t: back.at[c, t], ret.at[c], send_r.at[c], recv_r.at[c])
            ret[c, me] = back[c, me]

        @pl.when(c == 2)
        def _():
            for h, target in enumerate((ret_half, last_out)):
                give_back(lambda t: back.at[2, t, :, pl.ds(128 * h, 128)], target, send_r.at[2 + h], recv_r.at[2 + h])
                target[me] = back[2, me, :, pl.ds(128 * h, 128)]

        return 0

    lax.fori_loop(0, 3, filter_chunk, 0)

    def early(c, _):
        all_of(ret, c, recv_r)
        synthesise(ret[c].reshape(512, 256), tab_y, first_out.at[c])
        return 0

    lax.fori_loop(0, 2, early, 0)
    half_of(ret_half, 0, recv_r)
    synthesise(ret_half[...].reshape(512, 128), tab_y, second_out)

    def finish(c, _):
        all_of(spec, c, send_f)
        pltpu.make_async_copy(plane_out.at[c], plane_out.at[c], send_p.at[c]).wait()
        return 0

    lax.fori_loop(0, 3, finish, 0)
    for c in (0, 1):
        all_of(back, c, send_r)
    for h in (0, 1):
        half_of(ret_half, h, send_r)
    half_of(last_out, 1, recv_r)


def emit_kernel(first, second, last, tab_y, out, rest, sem):
    copies = [
        pltpu.make_async_copy(first, out.at[pl.ds(0, 2)], sem.at[0]),
        pltpu.make_async_copy(second, out.at[2, pl.ds(0, 128)], sem.at[1]),
        pltpu.make_async_copy(rest, out.at[2, pl.ds(128, 128)], sem.at[2]),
    ]
    copies[0].start()
    copies[1].start()
    synthesise(last[...].reshape(512, 128), tab_y, rest)
    copies[2].start()
    for copy in copies:
        copy.wait()


def in_hbm(array):
    return pltpu.with_memory_space_constraint(array, pltpu.HBM)


def on_device(velocity, cutoffs, plane_index, boundary_index):
    y_basis = half_basis(1024, KY).transpose(0, 1, 3, 2).reshape(2, 512, 512)
    x_basis = half_basis(2048, KX)
    x_back = x_basis.transpose(0, 1, 3, 2).reshape(2, 2, 512, 2, 512).transpose(0, 1, 3, 2, 4).reshape(8, 512, 512)
    tables = jnp.asarray(np.concatenate([y_basis, x_basis.reshape(8, 512, 512), x_back]))
    smem, vmem = pltpu.SMEM, pltpu.VMEM
    here = pl.BlockSpec(memory_space=vmem)
    anywhere = pl.BlockSpec(memory_space=pl.ANY)
    dma = pltpu.SemaphoreType.DMA
    blocks = vmem((3, SLABS, 8, 256), F32)
    scalar = pl.BlockSpec(memory_space=smem)
    pieces = pl.pallas_call(
        filter_kernel,
        out_shape=[
            jax.ShapeDtypeStruct((2, 256, 1024), F32),
            jax.ShapeDtypeStruct((128, 1024), F32),
            jax.ShapeDtypeStruct((SLABS, 8, 128), F32),
            jax.ShapeDtypeStruct((2, 512, 512), BF16),
        ],
        in_specs=[anywhere, anywhere, scalar, scalar, anywhere],
        out_specs=[here] * 4,
        scratch_shapes=[
            smem((1, 2, 8), jnp.int32),
            vmem((3, 256, 1024), F32),
            vmem((16, 512, 512), BF16),
            blocks,
            blocks,
            vmem((2, 128, 1024), BF16),
            vmem((2, 64, 512), F32),
            vmem((128, 512), BF16),
            vmem((2, 64, 1024), F32),
            vmem((2, 64, 1024), F32),
            blocks,
            vmem((2, SLABS, 8, 256), F32),
            vmem((SLABS, 8, 128), F32),
            vmem((16, 8, 128), F32),
            vmem((3, 64, 128), F32),
            vmem((3, 64, 128), F32),
        ]
        + [dma] + [dma((n,)) for n in (3, 3, 3, 3, 4, 4, 3, 3)],
        compiler_params=pltpu.CompilerParams(collective_id=0, has_side_effects=True, vmem_limit_bytes=VMEM_GRANT),
    )(in_hbm(velocity.reshape(3, 256, 1024)), in_hbm(cutoffs), plane_index, boundary_index, in_hbm(tables))
    out = pl.pallas_call(
        emit_kernel,
        out_shape=jax.ShapeDtypeStruct((3, 256, 1024), F32),
        in_specs=[here] * 4,
        out_specs=anywhere,
        scratch_shapes=[vmem((128, 1024), F32), dma((3,))],
        compiler_params=pltpu.CompilerParams(vmem_limit_bytes=16 << 20),
    )(*pieces)
    return out.reshape(velocity.shape)


def solution(mesh):
    in_specs = (P("ens", None, None, "slab", None), P("ens", None, None), P("ens"), P("ens"))
    out_specs = P("ens", None, None, "slab", None)
    return jax.shard_map(on_device, mesh=mesh, in_specs=in_specs, out_specs=out_specs, check_vma=False)
```

```python
import functools

import jax
import jax.numpy as jnp
import ml_dtypes
import numpy as np
from jax import lax
from jax.experimental import pallas as pl
from jax.experimental.pallas import tpu as pltpu
from jax.sharding import PartitionSpec as P

MESH = pl.DeviceIdType.MESH
KX = 512
KY = 256
SLABS = 64
FAR = 25
VMEM_GRANT = 36 << 20
AT_Y, AT_X, AT_XT = pl.ds(0, 2), pl.ds(2, 8), pl.ds(10, 8)
F32 = jnp.float32
BF16 = jnp.bfloat16


def split_table(table):
    high = table.astype(ml_dtypes.bfloat16)
    low = (table - high.astype(np.float64)).astype(ml_dtypes.bfloat16)
    return np.stack([high, low])


def half_basis(length, modes):
    position = np.arange(length // 2)
    tables = []
    for parity in (0, 1):
        wavenum = np.arange(parity, modes, 2)
        angles = (position[:, None] * wavenum[None, :] % length) * (2.0 * np.pi / length)
        tables.append(split_table(np.concatenate([np.cos(angles), np.sin(angles)], axis=1)))
    return np.stack(tables)


def dot(a, b):
    return lax.dot_general(a, b, (((1,), (0,)), ((), ())), preferred_element_type=F32)


def dot_nt(a, b):
    return lax.dot_general(a, b, (((1,), (1,)), ((), ())), preferred_element_type=F32)


def split(value):
    high = value.astype(BF16)
    return high, (value - high.astype(F32)).astype(BF16)


def synthesise(coefficients, tab_y, out):
    halves = []
    for parity in (0, 1):
        y_high, y_low = tab_y[parity, :256], tab_y[parity, 256:]
        high, low = split(coefficients[256 * parity : 256 * parity + 256].T)
        halves.append(dot(high, y_high) + (dot(low, y_high) + dot(high, y_low)))
    out[:, :512] = halves[0] + halves[1]
    out[:, 512:] = halves[0] - halves[1]


def exchange_groups(parts):
    lane = lax.broadcasted_iota(jnp.int32, parts[0].shape, parts[0].ndim - 1)
    axis = parts[0].ndim - 1
    for bit, width in ((1, 32), (2, 64)):
        first = (lane // width) % 2 == 0
        done = list(parts)
        for a in range(4):
            if a & bit:
                continue
            u, v = parts[a], parts[a | bit]
            done[a] = jnp.where(first, u, pltpu.roll(v, width, axis))
            done[a | bit] = jnp.where(first, pltpu.roll(u, 128 - width, axis), v)
        parts = done
    return parts


def filter_kernel(
    vel, cut_at, plane, bound, tables,
    first_out, second_out, last_out, tab_y,
    cut, u, tab, spec, recv, data, mask, coef, parts, field, back, ret, ret_half, relax, plane_out, plane_in,
    scalar, load, table, send_f, recv_f, send_r, recv_r, send_p, recv_p, ready,
):
    ens = lax.axis_index("ens")
    me = lax.axis_index("slab")
    my_y, my_z, my_c = lax.div(me, 16), lax.rem(lax.div(me, 2), 8), lax.rem(me, 2)
    after, before = lax.rem(ens + 1, 4), lax.rem(ens + 3, 4)

    def other(i):
        i = i - 1
        step = lax.div(i, 8)
        dz = lax.rem(12 + (1 - 2 * lax.rem(step, 2)) * lax.div(step + 1, 2), 8)
        dy, dc = 3 - lax.rem(lax.div(i, 2), 4), 1 - lax.rem(i, 2)
        return lax.rem(my_y + dy, 4) * 16 + lax.rem(my_z + dz, 8) * 2 + lax.rem(my_c + dc, 2)

    def served(i):
        step = lax.div(i, 8)
        z = step + lax.div(step, 5) * (12 - 2 * step)
        return lax.rem(my_y + lax.rem(lax.div(i, 2), 4), 4) * 16 + z * 2 + lax.rem(my_c + lax.rem(i, 2), 2)

    loads = [pltpu.make_async_copy(vel.at[c], u.at[c], load.at[c]) for c in range(3)]
    bases = [
        pltpu.make_async_copy(tables.at[AT_Y], tab_y, table.at[0]),
        pltpu.make_async_copy(tables.at[AT_X], tab.at[pl.ds(0, 8)], table.at[1]),
        pltpu.make_async_copy(tables.at[AT_XT], tab.at[pl.ds(8, 8)], table.at[2]),
    ]
    limits = pltpu.make_async_copy(cut_at, cut, scalar)
    loads[0].start()
    bases[0].start()

    barrier = pltpu.get_barrier_semaphore()

    def greet(i, _):
        pl.semaphore_signal(barrier, 1, device_id={"ens": ens, "slab": other(i)}, device_id_type=MESH)
        return 0

    lax.fori_loop(FAR, SLABS, greet, 0)
    for e in (after, before):
        pl.semaphore_signal(barrier, 1, device_id={"ens": e, "slab": me}, device_id_type=MESH)
    for copy in (loads[1], loads[2], bases[1], bases[2], limits):
        copy.start()

    def spread(source, target, c, sent, landed, first=1, end=SLABS):
        def one(i, _):
            t = other(i)
            pltpu.make_async_remote_copy(
                source.at[c, t], target.at[c, me], sent.at[c], landed.at[c],
                device_id={"ens": ens, "slab": t}, device_id_type=MESH,
            ).start()
            return 0

        lax.fori_loop(first, end, one, 0)

    def all_of(buffer, c, sem):
        blocks = buffer.at[c, pl.ds(0, SLABS - 1)]
        pltpu.make_async_copy(blocks, blocks, sem.at[c]).wait()

    def half_of(buffer, h, sem):
        blocks = buffer.at[pl.ds(0, SLABS - 1)]
        pltpu.make_async_copy(blocks, blocks, sem.at[2 + h]).wait()

    def give_back(source, target, sent, landed):
        def one(i, _):
            t = served(i)

            @pl.when(t != me)
            def _():
                pltpu.make_async_remote_copy(
                    source(t), target.at[me], sent, landed, device_id={"ens": ens, "slab": t}, device_id_type=MESH
                ).start()

            return 0

        lax.fori_loop(0, SLABS, one, 0)

    def analyse(c):
        pltpu.make_async_copy(vel.at[c], u.at[c], load.at[c]).wait()
        left, right = u[c, :, :512], u[c, :, 512:]
        for parity in (0, 1):
            high, low = split(left + right if parity == 0 else left - right)
            y_high, y_low = tab_y[parity, :256], tab_y[parity, 256:]
            total = dot_nt(y_high, high) + (dot_nt(y_high, low) + dot_nt(y_low, high))
            spec[c, pl.ds(32 * parity, 32)] = total.reshape(32, 8, 256)

    bases[0].wait()
    analyse(0)
    pl.semaphore_wait(barrier, SLABS - FAR + 2)
    for dz in (2, 6):
        there = my_y * 16 + lax.rem(my_z + dz, 8) * 2 + my_c
        pl.semaphore_signal(ready, 1, device_id={"ens": ens, "slab": there}, device_id_type=MESH)
    spread(spec, recv, 0, send_f, recv_f, FAR, SLABS)
    pl.semaphore_wait(ready, 2)
    spread(spec, recv, 0, send_f, recv_f, 1, FAR)
    recv[0, me] = spec[0, me]

    def forward(c, _):
        analyse(c)
        spread(spec, recv, c, send_f, recv_f)
        recv[c, me] = spec[c, me]
        return 0

    lax.fori_loop(1, 3, forward, 0)

    limits.wait()
    row = lax.broadcasted_iota(jnp.int32, (8, 512), 0)
    column = lax.broadcasted_iota(jnp.int32, (8, 512), 1)
    ky = 2 * ((8 * me + row) % 128) + lax.div(me, 32)
    weight_y = jnp.where(ky == 0, 1.0, 2.0) / 1024.0
    for parity in (0, 1):
        kx = 2 * (column % 256) + parity
        weight = weight_y * (jnp.where(kx == 0, 1.0, 2.0) / 2048.0)
        for z in range(8):
            kept = jnp.logical_and(kx <= cut[0, 0, z], ky <= cut[0, 1, z])
            mask[parity, pl.ds(8 * z, 8), :] = jnp.where(kept, weight, 0.0)
    lane = lax.broadcasted_iota(jnp.int32, (8, 128), 1)
    for q in range(16):
        offset = jnp.abs(128 * q + lane - bound[0])
        distance = jnp.minimum(offset, 2048 - offset)
        relax[q] = jnp.exp(-distance.astype(F32) / 512.0)
    bases[1].wait()
    bases[2].wait()

    def filter_chunk(c, _):
        all_of(recv, c, recv_f)

        def gather(q, _):
            at = pl.ds(pl.multiple_of(128 * q, 128), 128)
            for h in (0, 1):
                pieces = [(recv[c, 4 * q + a, :, pl.ds(128 * h, 128)], recv[c, 32 + 4 * q + a, :, pl.ds(128 * h, 128)]) for a in range(4)]
                for parity in (0, 1):
                    mixed = exchange_groups([m + n if parity == 0 else m - n for m, n in pieces])
                    high, low = split(jnp.concatenate(mixed, axis=0))
                    data[parity, pl.ds(32 * h, 32), at] = high
                    data[parity, pl.ds(64 + 32 * h, 32), at] = low
            return 0

        lax.fori_loop(0, 8, gather, 0)
        for parity in (0, 1):
            x_high, x_low = (tab[pl.ds(4 * parity + 2 * i, 2)].reshape(1024, 512) for i in (0, 1))
            both = dot(data[parity], x_high)
            kept = (both[:64] + (both[64:] + dot(data[parity, :64], x_low))) * mask[parity]
            high, low = split(kept)
            coef[:64] = high
            coef[64:] = low
            for side in (0, 1):
                both = dot(coef[...], tab[8 + 4 * parity + side])
                low = dot(coef[:64], tab[10 + 4 * parity + side])
                parts[parity, :, pl.ds(512 * side, 512)] = both[:64] + (both[64:] + low)

        xi = lax.broadcasted_iota(jnp.int32, (64, 128), 1)

        def combine(q, picked):
            at = pl.ds(pl.multiple_of(128 * q, 128), 128)
            even, odd = parts[0, :, at], parts[1, :, at]
            near, far = even + odd, even - odd
            field[0, :, at] = near
            field[1, :, at] = far
            x = xi + 128 * q
            return picked + (jnp.where(x == plane[0], near, 0.0) + jnp.where(x + 1024 == plane[0], far, 0.0))

        picked = lax.fori_loop(0, 8, combine, jnp.zeros((64, 128), F32))
        plane_out[c] = jnp.broadcast_to(jnp.sum(picked, axis=1, keepdims=True), (64, 128))
        handed = pltpu.make_async_remote_copy(
            plane_out.at[c], plane_in.at[c], send_p.at[c], recv_p.at[c],
            device_id={"ens": after, "slab": me}, device_id_type=MESH,
        )
        handed.start()
        handed.wait_recv()

        def scatter(q, _):
            at = pl.ds(pl.multiple_of(128 * q, 128), 128)
            for half in (0, 1):
                weight = relax[8 * half + q]
                for h in (0, 1):
                    rows = []
                    for b in range(4):
                        own = field[half, pl.ds(32 * h + 8 * b, 8), at]
                        rows.append(own + weight * (plane_in[c, pl.ds(32 * h + 8 * b, 8), :] - own))
                    for a, piece in enumerate(exchange_groups(rows)):
                        back[c, 32 * half + 4 * q + a, :, pl.ds(128 * h, 128)] = piece
            return 0

        lax.fori_loop(0, 8, scatter, 0)

        @pl.when(c < 2)
        def _():
            give_back(lambda t: back.at[c, t], ret.at[c], send_r.at[c], recv_r.at[c])
            ret[c, me] = back[c, me]

        @pl.when(c == 2)
        def _():
            for h, target in enumerate((ret_half, last_out)):
                give_back(lambda t: back.at[2, t, :, pl.ds(128 * h, 128)], target, send_r.at[2 + h], recv_r.at[2 + h])
                target[me] = back[2, me, :, pl.ds(128 * h, 128)]

        return 0

    lax.fori_loop(0, 3, filter_chunk, 0)

    def early(c, _):
        all_of(ret, c, recv_r)
        synthesise(ret[c].reshape(512, 256), tab_y, first_out.at[c])
        return 0

    lax.fori_loop(0, 2, early, 0)
    half_of(ret_half, 0, recv_r)
    synthesise(ret_half[...].reshape(512, 128), tab_y, second_out)

    def finish(c, _):
        all_of(spec, c, send_f)
        pltpu.make_async_copy(plane_out.at[c], plane_out.at[c], send_p.at[c]).wait()
        return 0

    lax.fori_loop(0, 3, finish, 0)
    for c in (0, 1):
        all_of(back, c, send_r)
    for h in (0, 1):
        half_of(ret_half, h, send_r)
    half_of(last_out, 1, recv_r)


def emit_kernel(first, second, last, tab_y, out, rest, sem):
    copies = [
        pltpu.make_async_copy(first, out.at[pl.ds(0, 2)], sem.at[0]),
        pltpu.make_async_copy(second, out.at[2, pl.ds(0, 128)], sem.at[1]),
        pltpu.make_async_copy(rest, out.at[2, pl.ds(128, 128)], sem.at[2]),
    ]
    copies[0].start()
    copies[1].start()
    synthesise(last[...].reshape(512, 128), tab_y, rest)
    copies[2].start()
    for copy in copies:
        copy.wait()


def in_hbm(array):
    return pltpu.with_memory_space_constraint(array, pltpu.HBM)


def on_device(velocity, cutoffs, plane_index, boundary_index):
    y_basis = half_basis(1024, KY).transpose(0, 1, 3, 2).reshape(2, 512, 512)
    x_basis = half_basis(2048, KX)
    x_back = x_basis.transpose(0, 1, 3, 2).reshape(2, 2, 512, 2, 512).transpose(0, 1, 3, 2, 4).reshape(8, 512, 512)
    tables = jnp.asarray(np.concatenate([y_basis, x_basis.reshape(8, 512, 512), x_back]))
    smem, vmem = pltpu.SMEM, pltpu.VMEM
    here = pl.BlockSpec(memory_space=vmem)
    anywhere = pl.BlockSpec(memory_space=pl.ANY)
    dma = pltpu.SemaphoreType.DMA
    blocks = vmem((3, SLABS, 8, 256), F32)
    scalar = pl.BlockSpec(memory_space=smem)
    pieces = pl.pallas_call(
        filter_kernel,
        out_shape=[
            jax.ShapeDtypeStruct((2, 256, 1024), F32),
            jax.ShapeDtypeStruct((128, 1024), F32),
            jax.ShapeDtypeStruct((SLABS, 8, 128), F32),
            jax.ShapeDtypeStruct((2, 512, 512), BF16),
        ],
        in_specs=[anywhere, anywhere, scalar, scalar, anywhere],
        out_specs=[here] * 4,
        scratch_shapes=[
            smem((1, 2, 8), jnp.int32),
            vmem((3, 256, 1024), F32),
            vmem((16, 512, 512), BF16),
            blocks,
            blocks,
            vmem((2, 128, 1024), BF16),
            vmem((2, 64, 512), F32),
            vmem((128, 512), BF16),
            vmem((2, 64, 1024), F32),
            vmem((2, 64, 1024), F32),
            blocks,
            vmem((2, SLABS, 8, 256), F32),
            vmem((SLABS, 8, 128), F32),
            vmem((16, 8, 128), F32),
            vmem((3, 64, 128), F32),
            vmem((3, 64, 128), F32),
        ]
        + [dma] + [dma((n,)) for n in (3, 3, 3, 3, 4, 4, 3, 3)] + [pltpu.SemaphoreType.REGULAR],
        compiler_params=pltpu.CompilerParams(collective_id=0, has_side_effects=True, vmem_limit_bytes=VMEM_GRANT),
    )(in_hbm(velocity.reshape(3, 256, 1024)), in_hbm(cutoffs), plane_index, boundary_index, in_hbm(tables))
    out = pl.pallas_call(
        emit_kernel,
        out_shape=jax.ShapeDtypeStruct((3, 256, 1024), F32),
        in_specs=[here] * 4,
        out_specs=anywhere,
        scratch_shapes=[vmem((128, 1024), F32), dma((3,))],
        compiler_params=pltpu.CompilerParams(vmem_limit_bytes=16 << 20),
    )(*pieces)
    return out.reshape(velocity.shape)


def solution(mesh):
    in_specs = (P("ens", None, None, "slab", None), P("ens", None, None), P("ens"), P("ens"))
    out_specs = P("ens", None, None, "slab", None)
    return jax.shard_map(on_device, mesh=mesh, in_specs=in_specs, out_specs=out_specs, check_vma=False)
```

```python
import functools

import jax
import jax.numpy as jnp
import ml_dtypes
import numpy as np
from jax import lax
from jax.experimental import pallas as pl
from jax.experimental.pallas import tpu as pltpu
from jax.sharding import PartitionSpec as P

MESH = pl.DeviceIdType.MESH
KX = 512
KY = 256
SLABS = 64
FAR = 25
VMEM_GRANT = 36 << 20
AT_Y, AT_X, AT_XT = pl.ds(0, 2), pl.ds(2, 8), pl.ds(10, 8)
F32 = jnp.float32
BF16 = jnp.bfloat16


def split_table(table):
    high = table.astype(ml_dtypes.bfloat16)
    low = (table - high.astype(np.float64)).astype(ml_dtypes.bfloat16)
    return np.stack([high, low])


def half_basis(length, modes):
    position = np.arange(length // 2)
    tables = []
    for parity in (0, 1):
        wavenum = np.arange(parity, modes, 2)
        angles = (position[:, None] * wavenum[None, :] % length) * (2.0 * np.pi / length)
        tables.append(split_table(np.concatenate([np.cos(angles), np.sin(angles)], axis=1)))
    return np.stack(tables)


def dot(a, b):
    return lax.dot_general(a, b, (((1,), (0,)), ((), ())), preferred_element_type=F32)


def dot_nt(a, b):
    return lax.dot_general(a, b, (((1,), (1,)), ((), ())), preferred_element_type=F32)


def split(value):
    high = value.astype(BF16)
    return high, (value - high.astype(F32)).astype(BF16)


def synthesise(coefficients, tab_y, out):
    halves = []
    for parity in (0, 1):
        y_high, y_low = tab_y[parity, :256], tab_y[parity, 256:]
        high, low = split(coefficients[256 * parity : 256 * parity + 256].T)
        halves.append(dot(high, y_high) + (dot(low, y_high) + dot(high, y_low)))
    out[:, :512] = halves[0] + halves[1]
    out[:, 512:] = halves[0] - halves[1]


def exchange_groups(parts):
    lane = lax.broadcasted_iota(jnp.int32, parts[0].shape, parts[0].ndim - 1)
    axis = parts[0].ndim - 1
    for bit, width in ((1, 32), (2, 64)):
        first = (lane // width) % 2 == 0
        done = list(parts)
        for a in range(4):
            if a & bit:
                continue
            u, v = parts[a], parts[a | bit]
            done[a] = jnp.where(first, u, pltpu.roll(v, width, axis))
            done[a | bit] = jnp.where(first, pltpu.roll(u, 128 - width, axis), v)
        parts = done
    return parts


def filter_kernel(
    vel, cut_at, plane, bound, tables,
    first_out, second_out, last_out, tab_y,
    cut, u, tab, spec, recv, data, mask, coef, parts, field, back, ret, ret_half, relax, plane_out, plane_in,
    scalar, load, table, send_f, recv_f, send_r, recv_r, send_p, recv_p, ready,
):
    ens = lax.axis_index("ens")
    me = lax.axis_index("slab")
    my_y, my_z, my_c = lax.div(me, 16), lax.rem(lax.div(me, 2), 8), lax.rem(me, 2)
    after, before = lax.rem(ens + 1, 4), lax.rem(ens + 3, 4)

    def other(i):
        i = i - 1
        step = lax.div(i, 8)
        dz = lax.rem(12 + (1 - 2 * lax.rem(step, 2)) * lax.div(step + 1, 2), 8)
        dy, dc = 3 - lax.rem(lax.div(i, 2), 4), 1 - lax.rem(i, 2)
        return lax.rem(my_y + dy, 4) * 16 + lax.rem(my_z + dz, 8) * 2 + lax.rem(my_c + dc, 2)

    def served(i):
        step = lax.div(i, 8)
        z = step + lax.div(step, 5) * (12 - 2 * step)
        return lax.rem(lax.div(i, 2), 4) * 16 + z * 2 + lax.rem(my_c + lax.rem(i, 2), 2)

    loads = [pltpu.make_async_copy(vel.at[c], u.at[c], load.at[c]) for c in range(3)]
    bases = [
        pltpu.make_async_copy(tables.at[AT_Y], tab_y, table.at[0]),
        pltpu.make_async_copy(tables.at[AT_X], tab.at[pl.ds(0, 8)], table.at[1]),
        pltpu.make_async_copy(tables.at[AT_XT], tab.at[pl.ds(8, 8)], table.at[2]),
    ]
    limits = pltpu.make_async_copy(cut_at, cut, scalar)
    loads[0].start()
    bases[0].start()

    barrier = pltpu.get_barrier_semaphore()

    def greet(i, _):
        pl.semaphore_signal(barrier, 1, device_id={"ens": ens, "slab": other(i)}, device_id_type=MESH)
        return 0

    lax.fori_loop(FAR, SLABS, greet, 0)
    for e in (after, before):
        pl.semaphore_signal(barrier, 1, device_id={"ens": e, "slab": me}, device_id_type=MESH)
    for copy in (loads[1], loads[2], bases[1], bases[2], limits):
        copy.start()

    def spread(source, target, c, sent, landed, first=1, end=SLABS):
        def one(i, _):
            t = other(i)
            pltpu.make_async_remote_copy(
                source.at[c, t], target.at[c, me], sent.at[c], landed.at[c],
                device_id={"ens": ens, "slab": t}, device_id_type=MESH,
            ).start()
            return 0

        lax.fori_loop(first, end, one, 0)

    def all_of(buffer, c, sem):
        blocks = buffer.at[c, pl.ds(0, SLABS - 1)]
        pltpu.make_async_copy(blocks, blocks, sem.at[c]).wait()

    def half_of(buffer, h, sem):
        blocks = buffer.at[pl.ds(0, SLABS - 1)]
        pltpu.make_async_copy(blocks, blocks, sem.at[2 + h]).wait()

    def give_back(source, target, sent, landed):
        def one(i, _):
            t = served(i)

            @pl.when(t != me)
            def _():
                pltpu.make_async_remote_copy(
                    source(t), target.at[me], sent, landed, device_id={"ens": ens, "slab": t}, device_id_type=MESH
                ).start()

            return 0

        lax.fori_loop(0, SLABS, one, 0)

    def analyse(c):
        pltpu.make_async_copy(vel.at[c], u.at[c], load.at[c]).wait()
        left, right = u[c, :, :512], u[c, :, 512:]
        for parity in (0, 1):
            high, low = split(left + right if parity == 0 else left - right)
            y_high, y_low = tab_y[parity, :256], tab_y[parity, 256:]
            total = dot_nt(y_high, high) + (dot_nt(y_high, low) + dot_nt(y_low, high))
            spec[c, pl.ds(32 * parity, 32)] = total.reshape(32, 8, 256)

    bases[0].wait()
    analyse(0)
    pl.semaphore_wait(barrier, SLABS - FAR + 2)
    for dz in (2, 6):
        there = my_y * 16 + lax.rem(my_z + dz, 8) * 2 + my_c
        pl.semaphore_signal(ready, 1, device_id={"ens": ens, "slab": there}, device_id_type=MESH)
    spread(spec, recv, 0, send_f, recv_f, FAR, SLABS)
    pl.semaphore_wait(ready, 2)
    spread(spec, recv, 0, send_f, recv_f, 1, FAR)
    recv[0, me] = spec[0, me]

    def forward(c, _):
        analyse(c)
        spread(spec, recv, c, send_f, recv_f)
        recv[c, me] = spec[c, me]
        return 0

    lax.fori_loop(1, 3, forward, 0)

    limits.wait()
    row = lax.broadcasted_iota(jnp.int32, (8, 512), 0)
    column = lax.broadcasted_iota(jnp.int32, (8, 512), 1)
    ky = 2 * ((8 * me + row) % 128) + lax.div(me, 32)
    weight_y = jnp.where(ky == 0, 1.0, 2.0) / 1024.0
    for parity in (0, 1):
        kx = 2 * (column % 256) + parity
        weight = weight_y * (jnp.where(kx == 0, 1.0, 2.0) / 2048.0)
        for z in range(8):
            kept = jnp.logical_and(kx <= cut[0, 0, z], ky <= cut[0, 1, z])
            mask[parity, pl.ds(8 * z, 8), :] = jnp.where(kept, weight, 0.0)
    lane = lax.broadcasted_iota(jnp.int32, (8, 128), 1)
    for q in range(16):
        offset = jnp.abs(128 * q + lane - bound[0])
        distance = jnp.minimum(offset, 2048 - offset)
        relax[q] = jnp.exp(-distance.astype(F32) / 512.0)
    bases[1].wait()
    bases[2].wait()

    def filter_chunk(c, _):
        all_of(recv, c, recv_f)

        def gather(q, _):
            at = pl.ds(pl.multiple_of(128 * q, 128), 128)
            for h in (0, 1):
                pieces = [(recv[c, 4 * q + a, :, pl.ds(128 * h, 128)], recv[c, 32 + 4 * q + a, :, pl.ds(128 * h, 128)]) for a in range(4)]
                for parity in (0, 1):
                    mixed = exchange_groups([m + n if parity == 0 else m - n for m, n in pieces])
                    high, low = split(jnp.concatenate(mixed, axis=0))
                    data[parity, pl.ds(32 * h, 32), at] = high
                    data[parity, pl.ds(64 + 32 * h, 32), at] = low
            return 0

        lax.fori_loop(0, 8, gather, 0)
        for parity in (0, 1):
            x_high, x_low = (tab[pl.ds(4 * parity + 2 * i, 2)].reshape(1024, 512) for i in (0, 1))
            both = dot(data[parity], x_high)
            kept = (both[:64] + (both[64:] + dot(data[parity, :64], x_low))) * mask[parity]
            high, low = split(kept)
            coef[:64] = high
            coef[64:] = low
            for side in (0, 1):
                both = dot(coef[...], tab[8 + 4 * parity + side])
                low = dot(coef[:64], tab[10 + 4 * parity + side])
                parts[parity, :, pl.ds(512 * side, 512)] = both[:64] + (both[64:] + low)

        xi = lax.broadcasted_iota(jnp.int32, (64, 128), 1)

        def combine(q, picked):
            at = pl.ds(pl.multiple_of(128 * q, 128), 128)
            even, odd = parts[0, :, at], parts[1, :, at]
            near, far = even + odd, even - odd
            field[0, :, at] = near
            field[1, :, at] = far
            x = xi + 128 * q
            return picked + (jnp.where(x == plane[0], near, 0.0) + jnp.where(x + 1024 == plane[0], far, 0.0))

        picked = lax.fori_loop(0, 8, combine, jnp.zeros((64, 128), F32))
        plane_out[c] = jnp.broadcast_to(jnp.sum(picked, axis=1, keepdims=True), (64, 128))
        handed = pltpu.make_async_remote_copy(
            plane_out.at[c], plane_in.at[c], send_p.at[c], recv_p.at[c],
            device_id={"ens": after, "slab": me}, device_id_type=MESH,
        )
        handed.start()
        handed.wait_recv()

        def scatter(q, _):
            at = pl.ds(pl.multiple_of(128 * q, 128), 128)
            for half in (0, 1):
                weight = relax[8 * half + q]
                for h in (0, 1):
                    rows = []
                    for b in range(4):
                        own = field[half, pl.ds(32 * h + 8 * b, 8), at]
                        rows.append(own + weight * (plane_in[c, pl.ds(32 * h + 8 * b, 8), :] - own))
                    for a, piece in enumerate(exchange_groups(rows)):
                        back[c, 32 * half + 4 * q + a, :, pl.ds(128 * h, 128)] = piece
            return 0

        lax.fori_loop(0, 8, scatter, 0)

        @pl.when(c < 2)
        def _():
            give_back(lambda t: back.at[c, t], ret.at[c], send_r.at[c], recv_r.at[c])
            ret[c, me] = back[c, me]

        @pl.when(c == 2)
        def _():
            for h, target in enumerate((ret_half, last_out)):
                give_back(lambda t: back.at[2, t, :, pl.ds(128 * h, 128)], target, send_r.at[2 + h], recv_r.at[2 + h])
                target[me] = back[2, me, :, pl.ds(128 * h, 128)]

        return 0

    lax.fori_loop(0, 3, filter_chunk, 0)

    def early(c, _):
        all_of(ret, c, recv_r)
        synthesise(ret[c].reshape(512, 256), tab_y, first_out.at[c])
        return 0

    lax.fori_loop(0, 2, early, 0)
    half_of(ret_half, 0, recv_r)
    synthesise(ret_half[...].reshape(512, 128), tab_y, second_out)

    def finish(c, _):
        all_of(spec, c, send_f)
        pltpu.make_async_copy(plane_out.at[c], plane_out.at[c], send_p.at[c]).wait()
        return 0

    lax.fori_loop(0, 3, finish, 0)
    for c in (0, 1):
        all_of(back, c, send_r)
    for h in (0, 1):
        half_of(ret_half, h, send_r)
    half_of(last_out, 1, recv_r)


def emit_kernel(first, second, last, tab_y, out, rest, sem):
    copies = [
        pltpu.make_async_copy(first, out.at[pl.ds(0, 2)], sem.at[0]),
        pltpu.make_async_copy(second, out.at[2, pl.ds(0, 128)], sem.at[1]),
        pltpu.make_async_copy(rest, out.at[2, pl.ds(128, 128)], sem.at[2]),
    ]
    copies[0].start()
    copies[1].start()
    synthesise(last[...].reshape(512, 128), tab_y, rest)
    copies[2].start()
    for copy in copies:
        copy.wait()


def in_hbm(array):
    return pltpu.with_memory_space_constraint(array, pltpu.HBM)


def on_device(velocity, cutoffs, plane_index, boundary_index):
    y_basis = half_basis(1024, KY).transpose(0, 1, 3, 2).reshape(2, 512, 512)
    x_basis = half_basis(2048, KX)
    x_back = x_basis.transpose(0, 1, 3, 2).reshape(2, 2, 512, 2, 512).transpose(0, 1, 3, 2, 4).reshape(8, 512, 512)
    tables = jnp.asarray(np.concatenate([y_basis, x_basis.reshape(8, 512, 512), x_back]))
    smem, vmem = pltpu.SMEM, pltpu.VMEM
    here = pl.BlockSpec(memory_space=vmem)
    anywhere = pl.BlockSpec(memory_space=pl.ANY)
    dma = pltpu.SemaphoreType.DMA
    blocks = vmem((3, SLABS, 8, 256), F32)
    scalar = pl.BlockSpec(memory_space=smem)
    pieces = pl.pallas_call(
        filter_kernel,
        out_shape=[
            jax.ShapeDtypeStruct((2, 256, 1024), F32),
            jax.ShapeDtypeStruct((128, 1024), F32),
            jax.ShapeDtypeStruct((SLABS, 8, 128), F32),
            jax.ShapeDtypeStruct((2, 512, 512), BF16),
        ],
        in_specs=[anywhere, anywhere, scalar, scalar, anywhere],
        out_specs=[here] * 4,
        scratch_shapes=[
            smem((1, 2, 8), jnp.int32),
            vmem((3, 256, 1024), F32),
            vmem((16, 512, 512), BF16),
            blocks,
            blocks,
            vmem((2, 128, 1024), BF16),
            vmem((2, 64, 512), F32),
            vmem((128, 512), BF16),
            vmem((2, 64, 1024), F32),
            vmem((2, 64, 1024), F32),
            blocks,
            vmem((2, SLABS, 8, 256), F32),
            vmem((SLABS, 8, 128), F32),
            vmem((16, 8, 128), F32),
            vmem((3, 64, 128), F32),
            vmem((3, 64, 128), F32),
        ]
        + [dma] + [dma((n,)) for n in (3, 3, 3, 3, 4, 4, 3, 3)] + [pltpu.SemaphoreType.REGULAR],
        compiler_params=pltpu.CompilerParams(collective_id=0, has_side_effects=True, vmem_limit_bytes=VMEM_GRANT),
    )(in_hbm(velocity.reshape(3, 256, 1024)), in_hbm(cutoffs), plane_index, boundary_index, in_hbm(tables))
    out = pl.pallas_call(
        emit_kernel,
        out_shape=jax.ShapeDtypeStruct((3, 256, 1024), F32),
        in_specs=[here] * 4,
        out_specs=anywhere,
        scratch_shapes=[vmem((128, 1024), F32), dma((3,))],
        compiler_params=pltpu.CompilerParams(vmem_limit_bytes=16 << 20),
    )(*pieces)
    return out.reshape(velocity.shape)


def solution(mesh):
    in_specs = (P("ens", None, None, "slab", None), P("ens", None, None), P("ens"), P("ens"))
    out_specs = P("ens", None, None, "slab", None)
    return jax.shard_map(on_device, mesh=mesh, in_specs=in_specs, out_specs=out_specs, check_vma=False)
```

```python
import functools

import jax
import jax.numpy as jnp
import ml_dtypes
import numpy as np
from jax import lax
from jax.experimental import pallas as pl
from jax.experimental.pallas import tpu as pltpu
from jax.sharding import PartitionSpec as P

MESH = pl.DeviceIdType.MESH
KX = 512
KY = 256
SLABS = 64
FAR = 25
VMEM_GRANT = 36 << 20
AT_Y, AT_X, AT_XT = pl.ds(0, 2), pl.ds(2, 8), pl.ds(10, 8)
F32 = jnp.float32
BF16 = jnp.bfloat16


def split_table(table):
    high = table.astype(ml_dtypes.bfloat16)
    low = (table - high.astype(np.float64)).astype(ml_dtypes.bfloat16)
    return np.stack([high, low])


def half_basis(length, modes):
    position = np.arange(length // 2)
    tables = []
    for parity in (0, 1):
        wavenum = np.arange(parity, modes, 2)
        angles = (position[:, None] * wavenum[None, :] % length) * (2.0 * np.pi / length)
        tables.append(split_table(np.concatenate([np.cos(angles), np.sin(angles)], axis=1)))
    return np.stack(tables)


def dot(a, b):
    return lax.dot_general(a, b, (((1,), (0,)), ((), ())), preferred_element_type=F32)


def dot_nt(a, b):
    return lax.dot_general(a, b, (((1,), (1,)), ((), ())), preferred_element_type=F32)


def split(value):
    high = value.astype(BF16)
    return high, (value - high.astype(F32)).astype(BF16)


def synthesise(coefficients, tab_y, out):
    halves = []
    for parity in (0, 1):
        y_high, y_low = tab_y[parity, :256], tab_y[parity, 256:]
        high, low = split(coefficients[256 * parity : 256 * parity + 256].T)
        halves.append(dot(high, y_high) + (dot(low, y_high) + dot(high, y_low)))
    out[:, :512] = halves[0] + halves[1]
    out[:, 512:] = halves[0] - halves[1]


def exchange_groups(parts):
    lane = lax.broadcasted_iota(jnp.int32, parts[0].shape, parts[0].ndim - 1)
    axis = parts[0].ndim - 1
    for bit, width in ((1, 32), (2, 64)):
        first = (lane // width) % 2 == 0
        done = list(parts)
        for a in range(4):
            if a & bit:
                continue
            u, v = parts[a], parts[a | bit]
            done[a] = jnp.where(first, u, pltpu.roll(v, width, axis))
            done[a | bit] = jnp.where(first, pltpu.roll(u, 128 - width, axis), v)
        parts = done
    return parts


def filter_kernel(
    vel, cut_at, plane, bound, tables,
    first_out, second_out, last_out, tab_y,
    cut, u, tab, spec, recv, data, mask, coef, parts, field, back, ret, ret_half, relax, plane_out, plane_in,
    scalar, load, table, send_f, recv_f, send_r, recv_r, send_p, recv_p, ready,
):
    ens = lax.axis_index("ens")
    me = lax.axis_index("slab")
    my_y, my_z, my_c = lax.div(me, 16), lax.rem(lax.div(me, 2), 8), lax.rem(me, 2)
    after, before = lax.rem(ens + 1, 4), lax.rem(ens + 3, 4)

    def other(i):
        i = i - 1
        step = lax.div(i, 8)
        dz = lax.rem(12 + (1 - 2 * lax.rem(step, 2)) * lax.div(step + 1, 2), 8)
        dy, dc = 3 - lax.rem(lax.div(i, 2), 4), 1 - lax.rem(i, 2)
        return lax.rem(my_y + dy, 4) * 16 + lax.rem(my_z + dz, 8) * 2 + lax.rem(my_c + dc, 2)

    def served(i):
        step = lax.div(i, 8)
        later = lax.div(step, 4)
        z = (1 - later) * lax.rem(6 - step, 4) + later * (11 - step)
        return lax.rem(lax.div(i, 2), 4) * 16 + z * 2 + lax.rem(my_c + lax.rem(i, 2), 2)

    loads = [pltpu.make_async_copy(vel.at[c], u.at[c], load.at[c]) for c in range(3)]
    bases = [
        pltpu.make_async_copy(tables.at[AT_Y], tab_y, table.at[0]),
        pltpu.make_async_copy(tables.at[AT_X], tab.at[pl.ds(0, 8)], table.at[1]),
        pltpu.make_async_copy(tables.at[AT_XT], tab.at[pl.ds(8, 8)], table.at[2]),
    ]
    limits = pltpu.make_async_copy(cut_at, cut, scalar)
    loads[0].start()
    bases[0].start()

    barrier = pltpu.get_barrier_semaphore()

    def greet(i, _):
        pl.semaphore_signal(barrier, 1, device_id={"ens": ens, "slab": other(i)}, device_id_type=MESH)
        return 0

    lax.fori_loop(FAR, SLABS, greet, 0)
    for e in (after, before):
        pl.semaphore_signal(barrier, 1, device_id={"ens": e, "slab": me}, device_id_type=MESH)
    for copy in (loads[1], loads[2], bases[1], bases[2], limits):
        copy.start()

    def spread(source, target, c, sent, landed, first=1, end=SLABS):
        def one(i, _):
            t = other(i)
            pltpu.make_async_remote_copy(
                source.at[c, t], target.at[c, me], sent.at[c], landed.at[c],
                device_id={"ens": ens, "slab": t}, device_id_type=MESH,
            ).start()
            return 0

        lax.fori_loop(first, end, one, 0)

    def all_of(buffer, c, sem):
        blocks = buffer.at[c, pl.ds(0, SLABS - 1)]
        pltpu.make_async_copy(blocks, blocks, sem.at[c]).wait()

    def half_of(buffer, h, sem):
        blocks = buffer.at[pl.ds(0, SLABS - 1)]
        pltpu.make_async_copy(blocks, blocks, sem.at[2 + h]).wait()

    def give_back(source, target, sent, landed):
        def one(i, _):
            t = served(i)

            @pl.when(t != me)
            def _():
                pltpu.make_async_remote_copy(
                    source(t), target.at[me], sent, landed, device_id={"ens": ens, "slab": t}, device_id_type=MESH
                ).start()

            return 0

        lax.fori_loop(0, SLABS, one, 0)

    def analyse(c):
        pltpu.make_async_copy(vel.at[c], u.at[c], load.at[c]).wait()
        left, right = u[c, :, :512], u[c, :, 512:]
        for parity in (0, 1):
            high, low = split(left + right if parity == 0 else left - right)
            y_high, y_low = tab_y[parity, :256], tab_y[parity, 256:]
            total = dot_nt(y_high, high) + (dot_nt(y_high, low) + dot_nt(y_low, high))
            spec[c, pl.ds(32 * parity, 32)] = total.reshape(32, 8, 256)

    bases[0].wait()
    analyse(0)
    pl.semaphore_wait(barrier, SLABS - FAR + 2)
    for dz in (2, 6):
        there = my_y * 16 + lax.rem(my_z + dz, 8) * 2 + my_c
        pl.semaphore_signal(ready, 1, device_id={"ens": ens, "slab": there}, device_id_type=MESH)
    spread(spec, recv, 0, send_f, recv_f, FAR, SLABS)
    pl.semaphore_wait(ready, 2)
    spread(spec, recv, 0, send_f, recv_f, 1, FAR)
    recv[0, me] = spec[0, me]

    def forward(c, _):
        analyse(c)
        spread(spec, recv, c, send_f, recv_f)
        recv[c, me] = spec[c, me]
        return 0

    lax.fori_loop(1, 3, forward, 0)

    limits.wait()
    row = lax.broadcasted_iota(jnp.int32, (8, 512), 0)
    column = lax.broadcasted_iota(jnp.int32, (8, 512), 1)
    ky = 2 * ((8 * me + row) % 128) + lax.div(me, 32)
    weight_y = jnp.where(ky == 0, 1.0, 2.0) / 1024.0
    for parity in (0, 1):
        kx = 2 * (column % 256) + parity
        weight = weight_y * (jnp.where(kx == 0, 1.0, 2.0) / 2048.0)
        for z in range(8):
            kept = jnp.logical_and(kx <= cut[0, 0, z], ky <= cut[0, 1, z])
            mask[parity, pl.ds(8 * z, 8), :] = jnp.where(kept, weight, 0.0)
    lane = lax.broadcasted_iota(jnp.int32, (8, 128), 1)
    for q in range(16):
        offset = jnp.abs(128 * q + lane - bound[0])
        distance = jnp.minimum(offset, 2048 - offset)
        relax[q] = jnp.exp(-distance.astype(F32) / 512.0)
    bases[1].wait()
    bases[2].wait()

    def filter_chunk(c, _):
        all_of(recv, c, recv_f)

        def gather(q, _):
            at = pl.ds(pl.multiple_of(128 * q, 128), 128)
            for h in (0, 1):
                pieces = [(recv[c, 4 * q + a, :, pl.ds(128 * h, 128)], recv[c, 32 + 4 * q + a, :, pl.ds(128 * h, 128)]) for a in range(4)]
                for parity in (0, 1):
                    mixed = exchange_groups([m + n if parity == 0 else m - n for m, n in pieces])
                    high, low = split(jnp.concatenate(mixed, axis=0))
                    data[parity, pl.ds(32 * h, 32), at] = high
                    data[parity, pl.ds(64 + 32 * h, 32), at] = low
            return 0

        lax.fori_loop(0, 8, gather, 0)
        for parity in (0, 1):
            x_high, x_low = (tab[pl.ds(4 * parity + 2 * i, 2)].reshape(1024, 512) for i in (0, 1))
            both = dot(data[parity], x_high)
            kept = (both[:64] + (both[64:] + dot(data[parity, :64], x_low))) * mask[parity]
            high, low = split(kept)
            coef[:64] = high
            coef[64:] = low
            for side in (0, 1):
                both = dot(coef[...], tab[8 + 4 * parity + side])
                low = dot(coef[:64], tab[10 + 4 * parity + side])
                parts[parity, :, pl.ds(512 * side, 512)] = both[:64] + (both[64:] + low)

        xi = lax.broadcasted_iota(jnp.int32, (64, 128), 1)

        def combine(q, picked):
            at = pl.ds(pl.multiple_of(128 * q, 128), 128)
            even, odd = parts[0, :, at], parts[1, :, at]
            near, far = even + odd, even - odd
            field[0, :, at] = near
            field[1, :, at] = far
            x = xi + 128 * q
            return picked + (jnp.where(x == plane[0], near, 0.0) + jnp.where(x + 1024 == plane[0], far, 0.0))

        picked = lax.fori_loop(0, 8, combine, jnp.zeros((64, 128), F32))
        plane_out[c] = jnp.broadcast_to(jnp.sum(picked, axis=1, keepdims=True), (64, 128))
        handed = pltpu.make_async_remote_copy(
            plane_out.at[c], plane_in.at[c], send_p.at[c], recv_p.at[c],
            device_id={"ens": after, "slab": me}, device_id_type=MESH,
        )
        handed.start()
        handed.wait_recv()

        def scatter(q, _):
            at = pl.ds(pl.multiple_of(128 * q, 128), 128)
            for half in (0, 1):
                weight = relax[8 * half + q]
                for h in (0, 1):
                    rows = []
                    for b in range(4):
                        own = field[half, pl.ds(32 * h + 8 * b, 8), at]
                        rows.append(own + weight * (plane_in[c, pl.ds(32 * h + 8 * b, 8), :] - own))
                    for a, piece in enumerate(exchange_groups(rows)):
                        back[c, 32 * half + 4 * q + a, :, pl.ds(128 * h, 128)] = piece
            return 0

        lax.fori_loop(0, 8, scatter, 0)

        @pl.when(c < 2)
        def _():
            give_back(lambda t: back.at[c, t], ret.at[c], send_r.at[c], recv_r.at[c])
            ret[c, me] = back[c, me]

        @pl.when(c == 2)
        def _():
            for h, target in enumerate((ret_half, last_out)):
                give_back(lambda t: back.at[2, t, :, pl.ds(128 * h, 128)], target, send_r.at[2 + h], recv_r.at[2 + h])
                target[me] = back[2, me, :, pl.ds(128 * h, 128)]

        return 0

    lax.fori_loop(0, 3, filter_chunk, 0)

    def early(c, _):
        all_of(ret, c, recv_r)
        synthesise(ret[c].reshape(512, 256), tab_y, first_out.at[c])
        return 0

    lax.fori_loop(0, 2, early, 0)
    half_of(ret_half, 0, recv_r)
    synthesise(ret_half[...].reshape(512, 128), tab_y, second_out)

    def finish(c, _):
        all_of(spec, c, send_f)
        pltpu.make_async_copy(plane_out.at[c], plane_out.at[c], send_p.at[c]).wait()
        return 0

    lax.fori_loop(0, 3, finish, 0)
    for c in (0, 1):
        all_of(back, c, send_r)
    for h in (0, 1):
        half_of(ret_half, h, send_r)
    half_of(last_out, 1, recv_r)


def emit_kernel(first, second, last, tab_y, out, rest, sem):
    copies = [
        pltpu.make_async_copy(first, out.at[pl.ds(0, 2)], sem.at[0]),
        pltpu.make_async_copy(second, out.at[2, pl.ds(0, 128)], sem.at[1]),
        pltpu.make_async_copy(rest, out.at[2, pl.ds(128, 128)], sem.at[2]),
    ]
    copies[0].start()
    copies[1].start()
    synthesise(last[...].reshape(512, 128), tab_y, rest)
    copies[2].start()
    for copy in copies:
        copy.wait()


def in_hbm(array):
    return pltpu.with_memory_space_constraint(array, pltpu.HBM)


def on_device(velocity, cutoffs, plane_index, boundary_index):
    y_basis = half_basis(1024, KY).transpose(0, 1, 3, 2).reshape(2, 512, 512)
    x_basis = half_basis(2048, KX)
    x_back = x_basis.transpose(0, 1, 3, 2).reshape(2, 2, 512, 2, 512).transpose(0, 1, 3, 2, 4).reshape(8, 512, 512)
    tables = jnp.asarray(np.concatenate([y_basis, x_basis.reshape(8, 512, 512), x_back]))
    smem, vmem = pltpu.SMEM, pltpu.VMEM
    here = pl.BlockSpec(memory_space=vmem)
    anywhere = pl.BlockSpec(memory_space=pl.ANY)
    dma = pltpu.SemaphoreType.DMA
    blocks = vmem((3, SLABS, 8, 256), F32)
    scalar = pl.BlockSpec(memory_space=smem)
    pieces = pl.pallas_call(
        filter_kernel,
        out_shape=[
            jax.ShapeDtypeStruct((2, 256, 1024), F32),
            jax.ShapeDtypeStruct((128, 1024), F32),
            jax.ShapeDtypeStruct((SLABS, 8, 128), F32),
            jax.ShapeDtypeStruct((2, 512, 512), BF16),
        ],
        in_specs=[anywhere, anywhere, scalar, scalar, anywhere],
        out_specs=[here] * 4,
        scratch_shapes=[
            smem((1, 2, 8), jnp.int32),
            vmem((3, 256, 1024), F32),
            vmem((16, 512, 512), BF16),
            blocks,
            blocks,
            vmem((2, 128, 1024), BF16),
            vmem((2, 64, 512), F32),
            vmem((128, 512), BF16),
            vmem((2, 64, 1024), F32),
            vmem((2, 64, 1024), F32),
            blocks,
            vmem((2, SLABS, 8, 256), F32),
            vmem((SLABS, 8, 128), F32),
            vmem((16, 8, 128), F32),
            vmem((3, 64, 128), F32),
            vmem((3, 64, 128), F32),
        ]
        + [dma] + [dma((n,)) for n in (3, 3, 3, 3, 4, 4, 3, 3)] + [pltpu.SemaphoreType.REGULAR],
        compiler_params=pltpu.CompilerParams(collective_id=0, has_side_effects=True, vmem_limit_bytes=VMEM_GRANT),
    )(in_hbm(velocity.reshape(3, 256, 1024)), in_hbm(cutoffs), plane_index, boundary_index, in_hbm(tables))
    out = pl.pallas_call(
        emit_kernel,
        out_shape=jax.ShapeDtypeStruct((3, 256, 1024), F32),
        in_specs=[here] * 4,
        out_specs=anywhere,
        scratch_shapes=[vmem((128, 1024), F32), dma((3,))],
        compiler_params=pltpu.CompilerParams(vmem_limit_bytes=16 << 20),
    )(*pieces)
    return out.reshape(velocity.shape)


def solution(mesh):
    in_specs = (P("ens", None, None, "slab", None), P("ens", None, None), P("ens"), P("ens"))
    out_specs = P("ens", None, None, "slab", None)
    return jax.shard_map(on_device, mesh=mesh, in_specs=in_specs, out_specs=out_specs, check_vma=False)
```
